512 devices in a mesh: seq: 128 (over x, z, y_lo), head: 4 (over y_hi, core).
Axes of the slice: x: 4, y: 8 (y_hi: 2, y_lo: 4; y = y_hi * 4 + y_lo), z: 8, core: 2. Of those that a mesh axis runs over, the one named last changes fastest.
Arguments:
- features: bfloat16 [32768, 1024], P('seq', 'head'), may hold values from -6 to 6
- w_query: bfloat16 [1024, 512], P(None, 'head'), may hold values from -0.1875 to 0.1875
- w_key: bfloat16 [1024, 512], P(None, 'head'), may hold values from -0.1875 to 0.1875
- w_value: bfloat16 [1024, 1024], P(None, 'head'), may hold values from -0.1875 to 0.1875
- w_gate: bfloat16 [1024, 1024], P(None, 'head'), may hold values from -0.1875 to 0.1875
- w_out: bfloat16 [1024, 1024], replicated, may hold values from -0.1875 to 0.1875
- forget: bfloat16 [2, 32768, 512], P(None, 'seq', 'head'), may hold values from -2.5 to 0, as said below
Outputs:
- encoded: bfloat16 [32768, 1024], P('seq', 'head')
The draws below stay inside these ranges and needn't reach their ends.
Inputs may be any that keep to these rules, and one draw needn't show every extreme that they name: `forget`: every entry is below zero.
All inputs are finite; a program needn't handle non-finite values.
Results may differ from the reference program's by a relative error of at most 0.013.
Values may be sent and summed in bfloat16 or wider, within the bound.
A program may use at most 64 MiB of HBM per device.

```python
import math
import jax
import jax.numpy as jnp
from jax import lax

D = 1024
HEADS = 8
HEAD_K = 64
HEAD_V = 128
GROUP = 64
TOK_DEV = 256
TOKENS = 32768
KEY_W = 512
VAL_W = 1024


def draw_forget(key, part):
    subkeys = jax.random.split(key, 7)
    slow_share = 0.5
    block_total = TOKENS // TOK_DEV
    slow_mask = jax.random.uniform(subkeys[0], (2, 1, 1, KEY_W)) < slow_share
    slow_rate = jnp.exp(jax.random.uniform(subkeys[1], (2, 1, 1, KEY_W), minval=math.log(0.1), maxval=0.0)) / TOKENS
    fast_rate = jnp.exp(jax.random.uniform(subkeys[2], (2, 1, 1, KEY_W), minval=math.log(1.0 / 400.0), maxval=math.log(1.0 / 30.0)))
    base_rate = jnp.where(slow_mask, slow_rate, fast_rate)
    device_factor = jnp.exp(jax.random.uniform(subkeys[3], (2, block_total, 1, KEY_W), minval=-math.log(2.0), maxval=math.log(2.0)))
    roughness = jax.random.uniform(subkeys[4], (2, block_total, TOK_DEV, KEY_W), minval=0.5, maxval=1.5)
    stable_level = (base_rate * device_factor * roughness).reshape(2, TOKENS, KEY_W)
    spots = jax.random.randint(subkeys[5], (2, 1, 3), 0, TOKENS)
    layer_depth_values = jax.random.uniform(subkeys[6], (2, 1, 3), minval=math.log(1.25), maxval=math.log(2.0))
    match_positions = (jnp.arange(TOKENS)[None, :, None] == spots).astype(jnp.float32)
    sudden_spikes = jnp.sum(match_positions * layer_depth_values, axis=2)[:, :, None]
    return (-(stable_level + sudden_spikes)).astype(jnp.bfloat16)


def block_scale(stream_key, shape, cuts, least, high):
    def one(position, parts):
        draws = jax.random.uniform(jax.random.fold_in(jax.random.fold_in(stream_key, 6), position), (parts,), jnp.float32, least / len(cuts), high / len(cuts))
        return jnp.repeat(jnp.exp(draws), shape[position] // parts).reshape((-1,) + (1,) * (len(shape) - position - 1))

    level = one(*cuts[0])
    for cut in cuts[1:]:
        level = level * one(*cut)
    return level


def normal_values(rng, dims, deviation, limit, cuts=(), kind=jnp.bfloat16):
    array = deviation * jax.random.normal(rng, dims, jnp.float32)
    if cuts:
        array = array * block_scale(rng, dims, cuts, -0.22, 0.18)
    return jnp.clip(array, -limit, limit).astype(kind)


def setup_inputs(seed: int = 0) -> dict:
    key_list = jax.random.split(jax.random.key(seed), 8)
    features = normal_values(key_list[0], (TOKENS, D), 1.0, 6.0, ((0, 128), (1, 4)))
    w_query = normal_values(key_list[1], (D, KEY_W), D ** -0.5, 0.1875, ((1, 4),))
    w_key = normal_values(key_list[2], (D, KEY_W), D ** -0.5, 0.1875, ((1, 4),))
    w_value = normal_values(key_list[3], (D, VAL_W), D ** -0.5, 0.1875, ((1, 4),))
    w_gate = normal_values(key_list[4], (D, VAL_W), D ** -0.5, 0.1875, ((1, 4),))
    w_out = normal_values(key_list[5], (VAL_W, D), VAL_W ** -0.5, 0.1875)
    forget = draw_forget(jax.random.fold_in(key_list[7], 71), 0)
    return {"features": features, "w_query": w_query, "w_key": w_key, "w_value": w_value, "w_gate": w_gate, "w_out": w_out, "forget": forget}


def block_pass(query_matrix, key_rows, value_rows, decays, initial):
    block_count = query_matrix.shape[0] // GROUP
    triangle = jnp.tril(jnp.ones((GROUP, GROUP), jnp.float32))

    def advance(memory, blocks):
        query_block, key_block, value_block, decay_block = blocks
        running = jnp.cumsum(decay_block, axis=0)
        query_decayed = (query_block.astype(jnp.float32) * jnp.exp(running)).astype(jnp.bfloat16).astype(jnp.float32)
        key_grown = (key_block.astype(jnp.float32) * jnp.exp(-running)).astype(jnp.bfloat16).astype(jnp.float32)
        value_float = value_block.astype(jnp.float32)
        scores = jnp.einsum('thi,shi->hts', query_decayed, key_grown, precision=lax.Precision.HIGHEST) * triangle
        scores = scores.astype(jnp.bfloat16).astype(jnp.float32)
        within = jnp.einsum('hts,shj->thj', scores, value_float, precision=lax.Precision.HIGHEST)
        carried = jnp.einsum('thi,hij->thj', query_decayed, memory, precision=lax.Precision.HIGHEST)
        finale = running[-1]
        key_to_end = (key_block.astype(jnp.float32) * jnp.exp(finale[None] - running)).astype(jnp.bfloat16).astype(jnp.float32)
        memory = jnp.exp(finale)[:, :, None] * memory + jnp.einsum('shi,shj->hij', key_to_end, value_float, precision=lax.Precision.HIGHEST)
        return (memory, within + carried)
    blocks = tuple((tensor.reshape((block_count, GROUP) + tensor.shape[1:]) for tensor in (query_matrix, key_rows, value_rows, decays)))
    last_memory, outputs = lax.scan(advance, initial, blocks)
    return outputs.reshape((block_count * GROUP,) + outputs.shape[2:])

def reference(features, w_query, w_key, w_value, w_gate, w_out, forget):
    query_matrix = (jnp.dot(features, w_query, preferred_element_type=jnp.float32) * 0.125).astype(jnp.bfloat16).reshape(TOKENS, HEADS, HEAD_K)
    key_rows = jnp.dot(features, w_key, preferred_element_type=jnp.float32).astype(jnp.bfloat16).reshape(TOKENS, HEADS, HEAD_K)
    value_rows = jnp.dot(features, w_value, preferred_element_type=jnp.float32).astype(jnp.bfloat16).reshape(TOKENS, HEADS, HEAD_V)
    gating = jnp.dot(features, w_gate, preferred_element_type=jnp.float32)
    decays = forget.astype(jnp.float32).reshape(2, TOKENS, HEADS, HEAD_K)
    blank_memory = jnp.zeros((HEADS, HEAD_K, HEAD_V), jnp.float32)
    ahead_out = block_pass(query_matrix, key_rows, value_rows, decays[0], blank_memory)
    behind_out = jnp.flip(block_pass(jnp.flip(query_matrix, 0), jnp.flip(key_rows, 0), jnp.flip(value_rows, 0), jnp.flip(decays[1], 0), blank_memory), 0)
    mixture = ahead_out + behind_out
    scaled = mixture * lax.rsqrt(lax.optimization_barrier(jnp.mean(mixture * mixture, axis=-1, keepdims=True)) + 1e-06)
    normed = (scaled.reshape(TOKENS, VAL_W) * jax.nn.silu(gating)).astype(jnp.bfloat16)
    return jnp.dot(normed, w_out, preferred_element_type=jnp.float32).astype(jnp.bfloat16)
```

```python
import functools

import jax
import jax.numpy as jnp
from jax import lax
from jax.experimental import pallas as pl
from jax.experimental.pallas import tpu as pltpu
from jax.sharding import Mesh
from jax.sharding import PartitionSpec as P

HEAD_K = 64
HEAD_V = 128
GROUP = 64
SEQ = ("x", "z", "yl")
HEAD = ("yh", "c")
MESH = pl.DeviceIdType.MESH
F32 = jnp.float32
BF16 = jnp.bfloat16
CHUNKS = 4


def dot(a, b, dims):
    return lax.dot_general(a, b, (dims, ((), ())), preferred_element_type=F32)


def mm(a, b):
    return dot(a, b, ((1,), (0,)))


def mm_t(a, b):
    return dot(a, b, ((1,), (1,)))


def t_mm(a, b):
    return dot(a, b, ((0,), (0,)))


def kernel(
    sizes,
    feats, wq, wk, wv, wg, wout, fg,
    out,
    fa, na, w, wo, fgv, acc, ex, kb, qb, vb, sg, base,
    y1s, y1r, ypre, zs, zr, xs, xr, y2s, y2r,
    load_sem, d_send, d_recv, r_send, r_recv, f_send, f_recv,
    y1_send, y1_recv, z_send, z_recv, x_send, x_recv, y2_send, y2_recv,
):
    nx, nz, ny = sizes
    tok, dcol = feats.shape
    kw = wq.shape[1]
    vw = wv.shape[1]
    pr = HEAD_V // ny
    rows = tok // CHUNKS
    blocks = tok // GROUP
    x, z, yl = lax.axis_index("x"), lax.axis_index("z"), lax.axis_index("yl")
    yh, c = lax.axis_index("yh"), lax.axis_index("c")
    h = yh * 2 + c
    h1 = yh * 2 + (1 - c)
    h2 = (1 - yh) * 2 + c
    h3 = (1 - yh) * 2 + (1 - c)

    def load(k, src, dst):
        return pltpu.make_async_copy(src, dst, load_sem.at[k])

    loads = [
        load(0, feats, fa.at[h]),
        load(1, fg, fgv),
        load(2, wk, w.at[:, pl.ds(0, kw)]),
        load(3, wv, w.at[:, pl.ds(kw, vw)]),
        load(4, wq, w.at[:, pl.ds(kw + vw, kw)]),
        load(5, wg, w.at[:, pl.ds(2 * kw + vw, vw)]),
        load(6, wout.at[:, pl.ds(pl.multiple_of(h * dcol, dcol), dcol)], wo),
    ]
    for item in loads:
        item.start()

    barrier = pltpu.get_barrier_semaphore()
    partners = [{"c": 1 - c}, {"yh": 1 - yh}]
    partners += [{"yl": lax.rem(yl + d, ny)} for d in range(1, ny)]
    partners += [{"z": lax.rem(z + d, nz)} for d in range(1, nz)]
    partners += [{"x": lax.rem(x + d, nx)} for d in range(1, nx)]
    for partner in partners:
        pl.semaphore_signal(barrier, inc=1, device_id=partner, device_id_type=MESH)
    pl.semaphore_wait(barrier, len(partners))

    def remote(src, dst, ss, rs, where):
        return pltpu.make_async_remote_copy(
            src_ref=src, dst_ref=dst, send_sem=ss, recv_sem=rs,
            device_id=where, device_id_type=MESH,
        )

    def part(buf, slot, n):
        return buf.at[slot, pl.ds(n * rows, rows)]

    core, across = {"c": 1 - c}, {"yh": 1 - yh}

    def direct(e, buf, n):
        piece = part(buf, h, n)
        return remote(piece, piece, d_send.at[e, n], d_recv.at[e, n], core)

    def far(e, buf, slot, n):
        piece = part(buf, slot, n)
        return remote(piece, piece, r_send.at[e, n], r_recv.at[e, n], across)

    def passed(e, buf, slot, n):
        piece = part(buf, slot, n)
        return remote(piece, piece, f_send.at[e, n], f_recv.at[e, n], core)

    def arrived_direct(e, buf, n):
        piece = part(buf, h1, n)
        remote(piece, piece, d_send.at[e, n], d_recv.at[e, n], core).wait_recv()

    loads[0].wait()
    for n in range(CHUNKS):
        far(0, fa, h, n).start()
    for n in range(CHUNKS):
        direct(0, fa, n).start()

    loads[1].wait()
    ti = lax.broadcasted_iota(jnp.int32, (tok, tok), 0)
    tj = lax.broadcasted_iota(jnp.int32, (tok, tok), 1)
    same = (ti // GROUP) == (tj // GROUP)

    def sums(mask, which):
        return mm(jnp.where(mask, 1.0, 0.0).astype(BF16), fgv[which])

    full = sums(tj <= ti, 0)
    total_f = full[tok - 1 : tok]
    ex[0] = jnp.exp(full)
    ex[1] = jnp.exp(sums(tj > ti, 0))
    inside = sums(same & (tj <= ti), 0)
    ex[2] = jnp.exp(inside)
    ex[3] = jnp.exp(-inside)
    ex[4] = jnp.exp(sums(same & (tj > ti), 0))
    full = sums(tj >= ti, 1)
    total_r = full[0:1]
    ex[5] = jnp.exp(full)
    ex[6] = jnp.exp(sums(tj < ti, 1))
    inside = sums(same & (tj >= ti), 1)
    ex[7] = jnp.exp(inside)
    ex[8] = jnp.exp(-inside)
    ex[9] = jnp.exp(sums(same & (tj < ti), 1))

    def packed(lf, lr):
        row = lax.broadcasted_iota(jnp.int32, (8, kw), 0)
        hf, hr = lf.astype(BF16).astype(F32), lr.astype(BF16).astype(F32)
        block = jnp.where(row == 0, hf, 0.0)
        block = jnp.where(row == 1, lf - hf, block)
        block = jnp.where(row == 2, hr, block)
        return jnp.where(row == 3, lr - hr, block).astype(BF16)

    def unpacked(ref, at):
        rows8 = ref[at, pl.ds(2 * pr, 8)].astype(F32)
        return rows8[0:1] + rows8[1:2], rows8[2:3] + rows8[3:4]

    for k in range(2, 6):
        loads[k].wait()

    def weights(slot):
        return pl.ds(pl.multiple_of(slot * dcol, dcol), dcol)

    acc[...] = mm(fa[h], w[weights(h)])
    for n in range(CHUNKS):
        arrived_direct(0, fa, n)
    acc[...] += mm(fa[h1], w[weights(h1)])

    kv = kw + vw
    for n in range(CHUNKS):
        far(0, fa, h2, n).wait_recv()
        passed(0, fa, h2, n).start()
        passed(0, fa, h3, n).wait_recv()
        span = pl.ds(n * rows, rows)
        got = (
            acc[span, pl.ds(0, kv)]
            + mm(fa[h2, span], w[weights(h2), pl.ds(0, kv)])
            + mm(fa[h3, span], w[weights(h3), pl.ds(0, kv)])
        )
        kb[span] = got[:, 0:kw].astype(BF16)
        vb[span] = got[:, kw:kv].astype(BF16)

    lane = lax.broadcasted_iota(jnp.int32, (HEAD_V, kw), 1)
    first = lane < HEAD_K

    def own_heads(both):
        top, low = both[0:HEAD_V], both[HEAD_V : 2 * HEAD_V]
        return (
            jnp.where(first, top[:, 0:kw], low[:, 0:kw]),
            jnp.where(first, top[:, kw : 2 * kw], low[:, kw : 2 * kw]),
        )

    keys = kb[...].astype(F32)
    ended = jnp.concatenate(
        [(keys * ex[1]).astype(BF16), (keys * ex[6]).astype(BF16)], axis=1
    )
    mem_f, mem_r = own_heads(t_mm(vb[...], ended))
    decay_rows = packed(total_f, total_r)
    for j in range(ny):
        y1s[j, pl.ds(0, pr)] = mem_f[j * pr : (j + 1) * pr].astype(BF16)
        y1s[j, pl.ds(pr, pr)] = mem_r[j * pr : (j + 1) * pr].astype(BF16)
        y1s[j, pl.ds(2 * pr, 8)] = decay_rows

    def to_all(n, me, axis, send, slot_of, recv, ss, rs):
        for d in range(1, n):
            to = lax.rem(me + d, n)
            remote(send.at[slot_of(to)], recv.at[me], ss.at[d], rs.at[me], {axis: to}).start()

    def from_all(n, me, axis, recv, ss, rs):
        for d in range(1, n):
            src = lax.rem(me + n - d, n)
            remote(recv.at[src], recv.at[src], ss.at[d], rs.at[src], {axis: src}).wait_recv()

    def sent_all(n, me, axis, send, slot_of, recv, ss, rs):
        for d in range(1, n):
            to = lax.rem(me + d, n)
            remote(send.at[slot_of(to)], recv.at[me], ss.at[d], rs.at[me], {axis: to}).wait_send()

    to_all(ny, yl, "yl", y1s, lambda to: to, y1r, y1_send, y1_recv)
    y1r[yl] = y1s[yl]

    qg = (
        acc[:, pl.ds(kv, kv)]
        + mm(fa[h2], w[weights(h2), pl.ds(kv, kv)])
        + mm(fa[h3], w[weights(h3), pl.ds(kv, kv)])
    )
    qb[...] = (qg[:, 0:kw] * 0.125).astype(BF16)
    gate = qg[:, kw:kv]
    sg[...] = gate / (1.0 + jnp.exp(-gate))

    from_all(ny, yl, "yl", y1r, y1_send, y1_recv)

    def walk(ref, order, which):
        state = jnp.zeros((pr, kw), F32)
        log = jnp.zeros((1, kw), F32)
        before = {}
        for j in order:
            before[j] = (state, log)
            step = unpacked(ref, j)[which]
            state = state * jnp.exp(step) + ref[j, pl.ds(which * pr, pr)].astype(F32)
            log = log + step
        return before, state, log

    before_f, state_f, log_f = walk(y1r, range(ny), 0)
    before_r, state_r, log_r = walk(y1r, range(ny)[::-1], 1)
    zs[pl.ds(0, pr)] = state_f.astype(BF16)
    zs[pl.ds(pr, pr)] = state_r.astype(BF16)
    zs[pl.ds(2 * pr, 8)] = packed(log_f, log_r)
    for d in range(1, nz):
        to = lax.rem(z + d, nz)
        remote(zs, zr.at[z], z_send.at[d], z_recv.at[z], {"z": to}).start()
    zr[z] = zs[...]

    queries = qb[...].astype(F32)
    keys = kb[...].astype(F32)
    qd = jnp.concatenate(
        [(queries * ex[2]).astype(BF16), (queries * ex[7]).astype(BF16)], axis=1
    )
    kd_f = (keys * ex[3]).astype(BF16)
    kd_r = (keys * ex[8]).astype(BF16)
    wide = lax.broadcasted_iota(jnp.int32, (tok, kw), 1) < HEAD_K
    ke = jnp.concatenate(
        [(keys * ex[4]).astype(BF16), (keys * ex[9]).astype(BF16)], axis=1
    )
    zero_b = jnp.zeros((), BF16)
    for head in range(2):
        mine = wide if head == 0 else jnp.logical_not(wide)
        s_f = mm_t(jnp.where(mine, qd[:, 0:kw], zero_b), kd_f)
        s_r = mm_t(jnp.where(mine, qd[:, kw : 2 * kw], zero_b), kd_r)
        scores = jnp.where(same & (tj <= ti), s_f, 0.0) + jnp.where(same & (tj >= ti), s_r, 0.0)
        span = pl.ds(head * HEAD_V, HEAD_V)
        base[:, span] = mm(scores.astype(BF16), vb[:, span])

    added = []
    for b in range(blocks):
        at = slice(b * GROUP, (b + 1) * GROUP)
        added.append(own_heads(t_mm(vb[at], ke[at])))
    held_f, held_r = {}, {}
    state = jnp.zeros((HEAD_V, kw), F32)
    for b in range(blocks):
        held_f[b] = state
        last = b * GROUP + GROUP - 1
        state = state * ex[2, last : last + 1] + added[b][0]
    state = jnp.zeros((HEAD_V, kw), F32)
    for b in range(blocks)[::-1]:
        held_r[b] = state
        last = b * GROUP
        state = state * ex[7, last : last + 1] + added[b][1]
    halves = lax.rem(lax.broadcasted_iota(jnp.int32, (HEAD_V, 2 * kw), 1), kw) < HEAD_K

    def split_heads(both):
        return jnp.concatenate(
            [jnp.where(halves, both, zero_b), jnp.where(halves, zero_b, both)], axis=0
        )

    for b in range(blocks):
        at = slice(b * GROUP, (b + 1) * GROUP)
        both = jnp.concatenate([held_f[b].astype(BF16), held_r[b].astype(BF16)], axis=1)
        base[at] += mm_t(qd[at], split_heads(both))

    for d in range(1, nz):
        src = lax.rem(z + nz - d, nz)
        remote(zr.at[src], zr.at[src], z_send.at[d], z_recv.at[src], {"z": src}).wait_recv()

    def reach(ref, n, me, which):
        state = ahead = jnp.zeros((pr, kw), F32)
        log = ahead_log = jnp.zeros((1, kw), F32)
        for k in range(n) if which == 0 else range(n)[::-1]:
            ahead = jnp.where(k == me, state, ahead)
            ahead_log = jnp.where(k == me, log, ahead_log)
            step = unpacked(ref, k)[which]
            state = state * jnp.exp(step) + ref[k, pl.ds(which * pr, pr)].astype(F32)
            log = log + step
        return ahead, ahead_log, state, log

    zf, zlog_f, state_f, log_f = reach(zr, nz, z, 0)
    zb, zlog_r, state_r, log_r = reach(zr, nz, z, 1)
    xs[pl.ds(0, pr)] = state_f.astype(BF16)
    xs[pl.ds(pr, pr)] = state_r.astype(BF16)
    xs[pl.ds(2 * pr, 8)] = packed(log_f, log_r)
    for d in range(1, nx):
        to = lax.rem(x + d, nx)
        remote(xs, xr.at[x], x_send.at[d], x_recv.at[x], {"x": to}).start()
    xr[x] = xs[...]
    for d in range(1, nx):
        src = lax.rem(x + nx - d, nx)
        remote(xr.at[src], xr.at[src], x_send.at[d], x_recv.at[src], {"x": src}).wait_recv()
    xf = reach(xr, nx, x, 0)[0]
    xb = reach(xr, nx, x, 1)[0]
    come_f = xf * jnp.exp(zlog_f) + zf
    come_r = xb * jnp.exp(zlog_r) + zb
    for j in range(ny):
        state, log = before_f[j]
        y2s[j, pl.ds(0, pr)] = (come_f * jnp.exp(log) + state).astype(BF16)
        state, log = before_r[j]
        y2s[j, pl.ds(pr, pr)] = (come_r * jnp.exp(log) + state).astype(BF16)
    to_all(ny, yl, "yl", y2s, lambda to: to, y2r, y2_send, y2_recv)
    y2r[yl] = y2s[yl]
    queries = qb[...].astype(F32)
    qx = jnp.concatenate(
        [(queries * ex[0]).astype(BF16), (queries * ex[5]).astype(BF16)], axis=1
    )
    from_all(ny, yl, "yl", y2r, y2_send, y2_recv)
    inflow = jnp.concatenate(
        [
            jnp.concatenate([y2r[j, pl.ds(0, pr)], y2r[j, pl.ds(pr, pr)]], axis=1)
            for j in range(ny)
        ],
        axis=0,
    )
    inflow = split_heads(inflow)

    for n in range(CHUNKS):
        at = slice(n * rows, (n + 1) * rows)
        mixed = base[at] + mm_t(qx[at], inflow)
        for head in range(2):
            span = slice(head * HEAD_V, (head + 1) * HEAD_V)
            mine = mixed[:, span]
            level = jnp.mean(mine * mine, axis=-1, keepdims=True)
            scaled = mine * lax.rsqrt(level + 1e-06)
            na[h, at, span] = (scaled * sg[at, span]).astype(BF16)
        far(1, na, h, n).start()
        direct(1, na, n).start()

    loads[6].wait()
    acc[:, pl.ds(0, dcol)] = mm(na[h], wo[weights(h)])
    for n in range(CHUNKS):
        arrived_direct(1, na, n)
    acc[:, pl.ds(0, dcol)] += mm(na[h1], wo[weights(h1)])
    for n in range(CHUNKS):
        far(1, na, h2, n).wait_recv()
        passed(1, na, h2, n).start()
        passed(1, na, h3, n).wait_recv()
        at = pl.ds(n * rows, rows)
        out[at] = (
            acc[at, pl.ds(0, dcol)]
            + mm(na[h2, at], wo[weights(h2)])
            + mm(na[h3, at], wo[weights(h3)])
        ).astype(BF16)

    for e, buf in ((0, fa), (1, na)):
        for n in range(CHUNKS):
            direct(e, buf, n).wait_send()
            far(e, buf, h, n).wait_send()
            passed(e, buf, h2, n).wait_send()
    sent_all(ny, yl, "yl", y1s, lambda to: to, y1r, y1_send, y1_recv)
    sent_all(ny, yl, "yl", y2s, lambda to: to, y2r, y2_send, y2_recv)
    for d in range(1, nz):
        to = lax.rem(z + d, nz)
        remote(zs, zr.at[z], z_send.at[d], z_recv.at[z], {"z": to}).wait_send()
    for d in range(1, nx):
        to = lax.rem(x + d, nx)
        remote(xs, xr.at[x], x_send.at[d], x_recv.at[x], {"x": to}).wait_send()


def local(sizes, features, w_query, w_key, w_value, w_gate, w_out, forget):
    nx, nz, ny = sizes
    tok, dcol = features.shape
    depth, kw = w_query.shape
    vw = w_value.shape[1]
    pr = HEAD_V // ny
    msg = 2 * pr + 8
    dma = pltpu.SemaphoreType.DMA
    return pl.pallas_call(
        functools.partial(kernel, sizes),
        out_shape=jax.ShapeDtypeStruct((tok, dcol), BF16),
        in_specs=[pl.BlockSpec(memory_space=pl.ANY)] * 7,
        out_specs=pl.BlockSpec(memory_space=pltpu.VMEM),
        scratch_shapes=[
            pltpu.VMEM((4, tok, dcol), BF16),
            pltpu.VMEM((4, tok, vw), BF16),
            pltpu.VMEM((depth, 2 * (kw + vw)), BF16),
            pltpu.VMEM((4 * vw, dcol), BF16),
            pltpu.VMEM((2, tok, kw), BF16),
            pltpu.VMEM((tok, 2 * (kw + vw)), F32),
            pltpu.VMEM((10, tok, kw), F32),
            pltpu.VMEM((tok, kw), BF16),
            pltpu.VMEM((tok, kw), BF16),
            pltpu.VMEM((tok, vw), BF16),
            pltpu.VMEM((tok, vw), F32),
            pltpu.VMEM((tok, vw), F32),
            pltpu.VMEM((ny, msg, kw), BF16),
            pltpu.VMEM((ny, msg, kw), BF16),
            pltpu.VMEM((8, kw), F32),
            pltpu.VMEM((msg, kw), BF16),
            pltpu.VMEM((nz, msg, kw), BF16),
            pltpu.VMEM((msg, kw), BF16),
            pltpu.VMEM((nx, msg, kw), BF16),
            pltpu.VMEM((ny, 2 * pr, kw), BF16),
            pltpu.VMEM((ny, 2 * pr, kw), BF16),
            dma((7,)),
            dma((2, CHUNKS)), dma((2, CHUNKS)),
            dma((2, CHUNKS)), dma((2, CHUNKS)),
            dma((2, CHUNKS)), dma((2, CHUNKS)),
            dma((ny,)), dma((ny,)),
            dma((nz,)), dma((nz,)),
            dma((nx,)), dma((nx,)),
            dma((ny,)), dma((ny,)),
        ],
        compiler_params=pltpu.CompilerParams(
            collective_id=0, has_side_effects=True, vmem_limit_bytes=60 * 1024 * 1024
        ),
        name="layer",
    )(features, w_query, w_key, w_value, w_gate, w_out, forget)


def solution(mesh, sizes=(4, 8, 4)):
    torus = Mesh(mesh.devices.reshape(*sizes, 2, 2), ("x", "z", "yl", "yh", "c"))
    placed = (
        P(SEQ, HEAD),
        P(None, HEAD),
        P(None, HEAD),
        P(None, HEAD),
        P(None, HEAD),
        P(),
        P(None, SEQ, HEAD),
    )
    return jax.shard_map(
        functools.partial(local, sizes),
        mesh=torus, in_specs=placed, out_specs=P(SEQ, HEAD), check_vma=False,
    )
```
